32 devices in a mesh: ctx: 8 (over z, x), tp: 4 (over y, core).
Axes of the slice: x: 2, y: 2, z: 4, core: 2. Of those that a mesh axis runs over, the one named last changes fastest.
Arguments:
- queries: bfloat16 [64, 4, 64, 128], P('ctx', None, 'tp'), may hold values from -250 to 250
- new_keys: bfloat16 [64, 4, 8, 128], P('ctx', None, 'tp'), may hold values from -6 to 6
- new_values: bfloat16 [64, 4, 8, 128], P('ctx', None, 'tp'), may hold values from -24 to 24
- key_pool: bfloat16 [512, 256, 8, 128], P('ctx', None, 'tp'), may hold values from -6 to 6
- value_pool: bfloat16 [512, 256, 8, 128], P('ctx', None, 'tp'), may hold values from -24 to 24
- slot_block: int32 [512], P('ctx'), may hold values from -1 to 8191, as said below
- lengths: int32 [64], replicated, may hold values from 1 to 32768, as said below
- out_weight: bfloat16 [8192, 8192], P('tp', 'ctx'), may hold values from -0.0625 to 0.0625
Outputs:
- layer_out: bfloat16 [64, 4, 8192], P('tp', None, 'ctx')
The draws below stay inside these ranges and needn't reach their ends.
Inputs may be any that keep to these rules, and one draw needn't show every extreme that they name: `slot_block`: each entry is r * 128 + j for block j of request r, or -1 for an empty slot. Every block j < b_r of every request r appears exactly once, where b_r = ceil(lengths[r] / 256). On each index of ctx the used slots come first. The owner of a request holds its first blocks as far as its slots reach; the remaining blocks lie on other indices of ctx. The blocks that one index of ctx holds of requests it does not own all belong to one request, and some index of ctx holds such blocks. `lengths`: some request has exactly 32768 positions.
All inputs are finite; a program needn't handle non-finite values.
Results may differ from the reference program's by a relative error of at most 0.006.
Values may be sent and summed in bfloat16 or wider, within the bound.
No kernel may reach another device: no remote copies, remote signals or barrier semaphores. Data moves between devices by JAX's collectives and lax.ppermute only.
A program may use at most 64 MiB of HBM per device.

```python
import jax
import jax.numpy as jnp
from jax import lax

D = 8192
HQ = 64
KVH = 8
HD = 128
R_DEV = 8
POOL = 64
STEPS = 4
BLK = 256
MAXB = 128
REQUESTS = 64
SLOTS = 512
N_CTX = 8


def placement(key):
    key = jax.random.fold_in(key, 7)
    key_a, key_b, key_c, key_d = jax.random.split(key, 4)
    request_count = N_CTX * R_DEV
    short_most = max(POOL // R_DEV // 4, 1)
    blocks = jax.random.randint(key_a, (request_count,), 1, short_most + 1).astype(jnp.int32)
    chosen_first = jax.random.randint(key_b, (), 0, request_count).astype(jnp.int32)
    chosen_second = ((chosen_first + (N_CTX // 2 + 2) % N_CTX * R_DEV) % request_count).astype(jnp.int32)
    chosen = jnp.stack([chosen_first, chosen_second]).astype(jnp.int32)
    long_size = jax.random.randint(key_c, (2,), POOL, MAXB + 1).astype(jnp.int32)
    long_size = long_size.at[0].set(MAXB)
    blocks = blocks.at[chosen].set(long_size)
    is_long = jnp.zeros((request_count,), jnp.bool_).at[chosen].set(True)
    tail_len = jax.random.randint(key_d, (request_count,), 1, BLK + 1).astype(jnp.int32)
    tail_len = tail_len.at[chosen[0]].set(BLK)
    lengths = ((blocks - 1) * BLK + tail_len).astype(jnp.int32)
    long_grid = is_long.reshape(N_CTX, R_DEV)
    per_owner = blocks.reshape(N_CTX, R_DEV)
    short_part = jnp.where(long_grid, 0, per_owner)
    long_part = jnp.where(long_grid, per_owner, 0)
    short_before = jnp.cumsum(short_part, axis=1) - short_part
    long_before = jnp.cumsum(long_part, axis=1) - long_part
    short_sum = jnp.sum(short_part, axis=1, keepdims=True)
    offsets = jnp.where(long_grid, short_sum + long_before, short_before).reshape(request_count).astype(jnp.int32)
    home_count = jnp.clip(POOL - offsets, 0, blocks).astype(jnp.int32)
    spill_count = (blocks - home_count).astype(jnp.int32)
    block_index = jnp.arange(MAXB, dtype=jnp.int32)
    local_pos = offsets[:, None] + block_index[None, :]
    present = block_index[None, :] < blocks[:, None]
    at_home = present & (local_pos < POOL)
    owners = jnp.arange(request_count, dtype=jnp.int32) // R_DEV
    code_grid = jnp.arange(request_count, dtype=jnp.int32)[:, None] * MAXB + block_index[None, :]
    slot_total = N_CTX * POOL
    slot_table = jnp.full((slot_total,), -1, jnp.int32)
    home_slot = jnp.where(at_home, owners[:, None] * POOL + local_pos, slot_total)
    slot_table = slot_table.at[home_slot.reshape(-1)].set(code_grid.reshape(-1), mode='drop')
    used_home = jnp.minimum(jnp.sum(per_owner, axis=1), POOL).astype(jnp.int32)
    capacity = (POOL - used_home).astype(jnp.int32)
    owner_first = (chosen_first // R_DEV).astype(jnp.int32)
    rank = jnp.arange(N_CTX, dtype=jnp.int32)
    stride = jnp.where(rank == 0, 1, jnp.where(rank == 1, N_CTX - 1, jnp.where(rank == N_CTX - 1, 0, rank))).astype(jnp.int32)
    lender_order = ((owner_first + stride) % N_CTX).astype(jnp.int32)
    room_left = capacity[lender_order]
    before = jnp.cumsum(room_left) - room_left
    long_first = chosen[0].astype(jnp.int32)
    long_second = chosen[1].astype(jnp.int32)
    lend_first = before < spill_count[long_first]
    end_first = jnp.sum(jnp.where(lend_first, room_left, 0))
    lend_second = (before >= end_first) & (before < end_first + spill_count[long_second])
    vacant = jnp.arange(POOL, dtype=jnp.int32)[None, :]
    fits_room = vacant < room_left[:, None]
    index_first = before[:, None] + vacant
    index_second = before[:, None] - end_first + vacant
    code_first = jnp.where(lend_first[:, None] & fits_room & (index_first < spill_count[long_first]), long_first * MAXB + home_count[long_first] + index_first, -1)
    code_second = jnp.where(lend_second[:, None] & fits_room & (index_second < spill_count[long_second]), long_second * MAXB + home_count[long_second] + index_second, -1)
    filling = jnp.maximum(code_first, code_second).astype(jnp.int32)
    target = jnp.where(filling >= 0, lender_order[:, None] * POOL + used_home[lender_order][:, None] + vacant, slot_total)
    slot_table = slot_table.at[target.reshape(-1)].set(filling.reshape(-1), mode='drop')
    return (lengths, slot_table)


def draw_lengths(key, part):
    return placement(key)[0]


def draw_slot_block(key, part):
    return placement(key)[1]


def draw_value_pool(key, part):
    key = jax.random.fold_in(key, 13)
    key_a, key_b = jax.random.split(key, 2)
    slot_total = N_CTX * POOL
    offset = jnp.clip(jax.random.normal(key_b, (slot_total, 1, KVH, HD), jnp.float32) * 3.0, -12.0, 12.0)
    noise = jnp.clip(jax.random.normal(key_a, (slot_total, BLK, KVH, HD), jnp.float32) * 3.0, -12.0, 12.0)
    return (noise + offset).astype(jnp.bfloat16)


def new_tokens(key):
    key = jax.random.fold_in(key, 11)
    key_a, key_b = jax.random.split(key, 2)
    request_count = N_CTX * R_DEV
    query = jnp.clip(jax.random.normal(key_a, (request_count, STEPS, HQ, HD), jnp.float32), -4.5, 4.5)
    gathered_keys = jnp.clip(jax.random.normal(key_b, (request_count, STEPS, KVH, HD), jnp.float32), -4.5, 4.5)
    return (query, gathered_keys)


def draw_queries(key, part):
    return new_tokens(key)[0].astype(jnp.bfloat16)


def draw_new_keys(key, part):
    return new_tokens(key)[1].astype(jnp.bfloat16)


def level_of(stream_key, shape, cuts, low, high):
    def one(axis_at, shards_of):
        draws = jax.random.uniform(jax.random.fold_in(jax.random.fold_in(stream_key, 6), axis_at), (shards_of,), jnp.float32, low / len(cuts), high / len(cuts))
        return jnp.repeat(jnp.exp(draws), shape[axis_at] // shards_of).reshape((-1,) + (1,) * (len(shape) - axis_at - 1))

    loudness = one(*cuts[0])
    for cut in cuts[1:]:
        loudness = loudness * one(*cut)
    return loudness


def centred(own_key, dims, scale, most, shards=(), kind=jnp.bfloat16):
    values = jax.random.normal(own_key, dims, jnp.float32) * scale
    if len(shards) > 0:
        values = level_of(own_key, dims, shards, -0.22, 0.18) * values
    return jnp.clip(values, min=-most, max=most).astype(kind)


def setup_inputs(seed: int = 0) -> dict:
    key_of = jax.random.split(jax.random.key(seed), 9)
    return {
        "queries": draw_queries(jax.random.fold_in(key_of[8], 71), 0),
        "new_keys": draw_new_keys(jax.random.fold_in(key_of[8], 71), 0),
        "new_values": centred(key_of[2], (REQUESTS, STEPS, KVH, HD), 4.0, 24.0, ((0, 8), (2, 4))),
        "key_pool": centred(key_of[3], (SLOTS, BLK, KVH, HD), 1.0, 6.0, ((0, 8), (2, 4))),
        "value_pool": draw_value_pool(jax.random.fold_in(key_of[8], 71), 0),
        "slot_block": draw_slot_block(jax.random.fold_in(key_of[8], 71), 0),
        "lengths": draw_lengths(jax.random.fold_in(key_of[8], 71), 0),
        "out_weight": centred(key_of[7], (HQ * HD, D), (HQ * HD) ** -0.5, 0.0625, ((0, 4), (1, 8))),
    }


def partial_block(decode_query_rows, gathered_keys, gathered_values, usable):
    head_width_size = decode_query_rows.shape[-1]
    logit_scores = jnp.einsum("rena,hea->enrh", decode_query_rows.astype(jnp.float32), gathered_keys.astype(jnp.float32)) * (head_width_size ** -0.5)
    masked = jnp.where(usable[None, None], logit_scores, jnp.float32(-1e30))
    highest = jnp.max(masked, axis=-1)
    softmax_weights = jnp.where(usable[None, None], jnp.exp(masked - highest[..., None]), jnp.float32(0.0)).astype(jnp.bfloat16)
    totals = jnp.sum(softmax_weights.astype(jnp.float32), axis=-1)
    weighted_sum = jnp.einsum("oywp,poa->oywa", softmax_weights.astype(jnp.float32), gathered_values.astype(jnp.float32))
    return highest.reshape(-1), totals.reshape(-1), weighted_sum.reshape(-1, head_width_size)


def reference(queries, new_keys, new_values, key_pool, value_pool, slot_block, lengths, out_weight):
    request_count, step_count, head_count, head_width_size = queries.shape
    kv_heads = new_keys.shape[2]
    group_size = head_count // kv_heads
    block_len = key_pool.shape[1]
    grouped = queries.reshape(request_count, step_count, kv_heads, group_size, head_width_size)

    def one_slot(items):
        code, gathered_keys, gathered_values = items
        in_use = code >= 0
        request = jnp.where(in_use, code // MAXB, 0).astype(jnp.int32)
        start_pos = (code % MAXB) * block_len
        position = start_pos + jnp.arange(block_len, dtype=jnp.int32)
        usable = in_use & (position < lengths[request])
        usable = jnp.broadcast_to(usable[None, :], (step_count, block_len))
        return partial_block(grouped[request], gathered_keys, gathered_values, usable)

    highest, totals, weighted_sum = lax.map(one_slot, (slot_block, key_pool, value_pool))
    in_use = slot_block >= 0
    request = jnp.where(in_use, slot_block // MAXB, 0).astype(jnp.int32)
    row_width = highest.shape[1]
    req_high = jnp.full((request_count, row_width), -1e30, jnp.float32).at[request].max(highest)
    factor = jnp.exp(highest - req_high[request])
    req_total = jax.ops.segment_sum(totals * factor, request, request_count)
    req_sum = jax.ops.segment_sum(weighted_sum * factor[..., None], request, request_count)
    causal = jnp.arange(step_count)[:, None] >= jnp.arange(step_count)[None, :]
    own_high, own_total, own_sum = jax.vmap(partial_block, in_axes=(0, 0, 0, None))(grouped, new_keys, new_values, causal)
    peak_all = jnp.maximum(req_high, own_high)
    left_factor = jnp.exp(req_high - peak_all)
    right_factor = jnp.exp(own_high - peak_all)
    denominator = req_total * left_factor + own_total * right_factor
    numerator = req_sum * left_factor[..., None] + own_sum * right_factor[..., None]
    attention = (numerator / denominator[..., None]).reshape(request_count, kv_heads, group_size, step_count, head_width_size)
    attention = attention.transpose(0, 3, 1, 2, 4).reshape(request_count * step_count, head_count * head_width_size).astype(jnp.bfloat16)
    projected = jnp.dot(attention, out_weight, preferred_element_type=jnp.float32)
    return projected.astype(jnp.bfloat16).reshape(request_count, step_count, -1)
```

```python
import functools
import math

import jax
import jax.numpy as jnp
from jax import lax
from jax.experimental import pallas as pl
from jax.experimental.pallas import tpu as pltpu
from jax.sharding import PartitionSpec as P

MAXB = 128
GROUP = 4
NEG = -1e30
LOG2E = math.log2(math.e)
F32 = jnp.float32
BF16 = jnp.bfloat16

NT = (((1,), (1,)), ((), ()))


def request_kernel(owned, rows, block_len, round_ref, slot_ref, len_ref, q_ref, out_ref, count):
    me = lax.axis_index("ctx")
    for r in range(owned):
        count[r] = 0

    def tally(s, carry):
        code = slot_ref[s]
        local = lax.div(code, MAXB) - me * owned

        @pl.when((code >= 0) & (local >= 0) & (local < owned))
        def _():
            count[local] = count[local] + 1

        return carry

    lax.fori_loop(0, slot_ref.shape[0], tally, 0)
    seen = jnp.int32(0)
    pick = jnp.int32(-1)
    for r in range(owned):
        blocks = lax.div(len_ref[me * owned + r] + (block_len - 1), block_len)
        lent = count[r] < blocks
        pick = jnp.where(lent & (seen == round_ref[0]), r, pick)
        seen = seen + lent.astype(jnp.int32)
    row = lax.broadcasted_iota(jnp.int32, (16, 128), 0)
    info = jnp.where(row == 0, seen, pick).astype(F32).astype(BF16)
    body = q_ref[jnp.maximum(pick, 0)]
    for c in range(out_ref.shape[0]):
        out_ref[c, pl.ds(0, rows), :] = body
        out_ref[c, pl.ds(rows, 16), :] = info


def attend(
    foreign, owned, kv, group, slot_ref, len_ref, query_of,
    k_hbm, v_hbm, kbuf, vbuf, ksem, vsem, order, m_acc, l_acc, a_acc,
):
    me = lax.axis_index("ctx")
    width, head = kbuf.shape[1:]
    block_len = width // kv
    rows = m_acc.shape[1]
    heads = group * kv
    coef = head ** -0.5 * LOG2E

    def begin(s, n):
        code = slot_ref[s]
        is_own = lax.div(lax.div(code, MAXB), owned) == me
        mine = (code >= 0) & (jnp.logical_not(is_own) if foreign else is_own)

        @pl.when(mine)
        def _():
            order[n] = s
            pltpu.make_async_copy(k_hbm.at[s], kbuf.at[n], ksem.at[n]).start()
            pltpu.make_async_copy(v_hbm.at[s], vbuf.at[n], vsem.at[n]).start()

        return n + mine.astype(jnp.int32)

    n = lax.fori_loop(0, slot_ref.shape[0], begin, jnp.int32(0))
    col = lax.broadcasted_iota(jnp.int32, (rows, width), 1)
    row = lax.broadcasted_iota(jnp.int32, (rows, width), 0)
    same = (col % kv) == (row % heads) // group
    place = jnp.where(same, col, width * 2)

    def step(it, carry):
        for g in range(GROUP):
            i = it * GROUP + g

            @pl.when(i < n)
            def _():
                pltpu.make_async_copy(k_hbm.at[0], kbuf.at[i], ksem.at[i]).wait()
                pltpu.make_async_copy(v_hbm.at[0], vbuf.at[i], vsem.at[i]).wait()

        parts = []
        for g in range(GROUP):
            i = it * GROUP + g
            slot = jnp.minimum(i, n - 1)
            code = slot_ref[order[slot]]
            r = lax.div(code, MAXB)
            valid = jnp.clip(len_ref[r] - (code - r * MAXB) * block_len, 0, block_len)
            valid = jnp.where(i < n, valid, 0) * kv
            e = jnp.int32(0) if foreign else r - me * owned
            scores = lax.dot_general(query_of(e), kbuf[slot], NT, preferred_element_type=F32)
            scores = jnp.where(place < valid, scores, NEG)
            high = jnp.max(scores, axis=1, keepdims=True)
            weights = jnp.exp2((scores - high) * coef).astype(BF16)
            rounded = weights.astype(F32)
            total = rounded[:, :128]
            for c in range(1, width // 128):
                total = total + rounded[:, c * 128 : (c + 1) * 128]
            summed = jnp.dot(weights, vbuf[slot], preferred_element_type=F32)
            parts.append((e, high, total, summed))
        for e, high, total, summed in parts:
            before = m_acc[e]
            peak = jnp.maximum(before, high)
            keep = jnp.exp2((before - peak) * coef)
            add = jnp.exp2((high - peak) * coef)
            m_acc[e] = peak
            l_acc[e] = l_acc[e] * keep + total * add
            a_acc[e] = a_acc[e] * keep + summed * add
        return carry

    lax.fori_loop(0, lax.div(n + GROUP - 1, GROUP), step, 0)
    return n


def own_kernel(
    owned, steps, kv, group, slot_ref, len_ref, q_ref, nk_ref, nv_ref, k_hbm, v_hbm,
    out_ref, lse_ref, kbuf, vbuf, ksem, vsem, order, m_acc, l_acc, a_acc,
):
    rows, head = q_ref.shape[1:]
    heads = kv * group
    coef = head ** -0.5 * LOG2E
    fresh = nk_ref.shape[0]
    col = lax.broadcasted_iota(jnp.int32, (rows, fresh), 1)
    row = lax.broadcasted_iota(jnp.int32, (rows, fresh), 0)
    seen = ((col % kv) == (row % heads) // group) & (lax.div(col, kv) % steps <= lax.div(row, heads))
    lane = lax.broadcasted_iota(jnp.int32, (rows, 128), 1)
    nk = nk_ref[...]
    nv = nv_ref[...]
    for r in range(owned):
        scores = lax.dot_general(q_ref[r], nk, NT, preferred_element_type=F32)
        ok = seen & (lax.div(col, kv * steps) == r)
        scores = jnp.where(ok, scores, NEG)
        high = jnp.max(scores, axis=1, keepdims=True)
        weights = jnp.where(ok, jnp.exp2((scores - high) * coef), 0.0).astype(BF16)
        total = jnp.sum(weights.astype(F32), axis=1, keepdims=True)
        m_acc[r] = jnp.broadcast_to(high, (rows, 128))
        l_acc[r] = jnp.where(lane == 0, total, 0.0)
        a_acc[r] = jnp.dot(weights, nv, preferred_element_type=F32)
    attend(
        False, owned, kv, group, slot_ref, len_ref, lambda e: q_ref[e],
        k_hbm, v_hbm, kbuf, vbuf, ksem, vsem, order, m_acc, l_acc, a_acc,
    )
    table = jnp.zeros((rows, 128), F32)
    for r in range(owned):
        total = jnp.sum(l_acc[r], axis=1, keepdims=True)
        out_ref[r] = (a_acc[r] / total).astype(BF16)
        table = jnp.where(lane % 32 == r, m_acc[r] * coef + jnp.log(total) * LOG2E, table)
    lse_ref[...] = table


def lent_kernel(
    owned, kv, group, slot_ref, len_ref, got_ref, lse_ref, k_hbm, v_hbm,
    out_ref, kbuf, vbuf, ksem, vsem, order, m_acc, l_acc, a_acc,
):
    rows, head = out_ref.shape[1:]
    coef = head ** -0.5 * LOG2E
    me = lax.axis_index("ctx")

    def find(s, rid):
        code = slot_ref[s]
        r = lax.div(code, MAXB)
        return jnp.where((code >= 0) & (lax.div(r, owned) != me), r, rid)

    rid = lax.fori_loop(0, slot_ref.shape[0], find, jnp.int32(0))
    owner = lax.div(rid, owned)
    m_acc[0] = jnp.full((rows, 128), NEG, F32)
    l_acc[0] = jnp.zeros((rows, 128), F32)
    a_acc[0] = jnp.zeros((rows, head), F32)
    attend(
        True, owned, kv, group, slot_ref, len_ref, lambda e: got_ref[owner, pl.ds(0, rows), :],
        k_hbm, v_hbm, kbuf, vbuf, ksem, vsem, order, m_acc, l_acc, a_acc,
    )
    total = jnp.sum(l_acc[0], axis=1, keepdims=True)
    some = total > 0.0
    total = jnp.where(some, total, 1.0)
    out_ref[0] = (a_acc[0] / total).astype(BF16)
    lse = jnp.where(some, m_acc[0] * coef + jnp.log(total) * LOG2E, NEG)
    lane = lax.broadcasted_iota(jnp.int32, (rows, 128), 1)
    table = jnp.where(lane % 32 == owned, lse, lse_ref[...])
    table = jnp.where(lane % 32 == owned + 1, rid.astype(F32), table)
    second = table - table.astype(BF16).astype(F32)
    third = second - second.astype(BF16).astype(F32)
    out_ref[1] = jnp.where(lane < 32, table, jnp.where(lane < 64, second, third)).astype(BF16)


def project_kernel(
    owned, steps, heads, sources, parts, lent_ref, *refs
):
    pieces = refs[:sources]
    w_hbm, send_ref, keep_ref, full, lse, flat, wbuf, wsem = refs[sources:]
    me = lax.axis_index("ctx")
    mine = lax.axis_index("tp")
    rows = steps * heads
    head = full.shape[1]
    span = owned * rows
    per = sources // parts
    copy = pltpu.make_async_copy(w_hbm, wbuf, wsem)
    copy.start()

    def spot(c):
        return (lax.div(c, per) ^ mine) * per + lax.rem(c, per)

    lane = lax.broadcasted_iota(jnp.int32, (rows, 128), 1)
    for d in range(sources):
        start = pl.multiple_of(spot(me ^ d) * span, span)
        full[pl.ds(start, span), :] = pieces[d][...].astype(F32).reshape(span, head)
    rids = []
    for d in range(sources):
        packed = lent_ref[d, 1].astype(F32)
        table = packed + pltpu.roll(packed, 96, 1) + pltpu.roll(packed, 64, 1)
        lse[d] = table
        rids.append(jnp.max(jnp.where(lane[:8] == owned + 1, table[:8], -1.0)).astype(jnp.int32))
    for d in range(sources):
        c = lax.div(rids[d], owned)
        r = lax.rem(rids[d], owned)
        start = pl.multiple_of((spot(c) * owned + r) * rows, rows)
        theirs = lse[c]
        left = jnp.sum(jnp.where(lane == r, theirs, 0.0), axis=1, keepdims=True)
        right = jnp.sum(jnp.where(lane == owned, lse[d], 0.0), axis=1, keepdims=True)
        peak = jnp.maximum(left, right)
        w_left = jnp.exp2(left - peak)
        w_right = jnp.exp2(right - peak)
        total = w_left + w_right
        full[pl.ds(start, rows), :] = full[pl.ds(start, rows), :] * (w_left / total) + lent_ref[
            d, 0
        ].astype(F32) * (w_right / total)
        lse[c] = jnp.where(lane == r, peak + jnp.log(total) * LOG2E, theirs)
    count = sources * owned * steps
    for h in range(heads):
        flat[:, h * head : (h + 1) * head] = full[pl.ds(h, count, stride=heads), :].astype(BF16)
    copy.wait()
    result = jnp.dot(flat[...], wbuf[...], preferred_element_type=F32).astype(BF16)
    kept = count // parts
    for b in range(parts):
        target = keep_ref if b % 2 == 0 else send_ref
        target[b // 2] = result[b * kept : (b + 1) * kept]


def smem():
    return pl.BlockSpec(memory_space=pltpu.SMEM)


def vmem():
    return pl.BlockSpec(memory_space=pltpu.VMEM)


def hbm():
    return pl.BlockSpec(memory_space=pltpu.HBM)


def per_device(
    queries, new_keys, new_values, key_pool, value_pool, slot_block, lengths, out_weight
):
    owned, steps, heads, head = queries.shape
    kv = new_keys.shape[2]
    group = heads // kv
    slots, block_len = key_pool.shape[:2]
    sources = lax.axis_size("ctx")
    parts = lax.axis_size("tp")
    rows = steps * heads
    cols = out_weight.shape[1]
    q = queries.reshape(owned, rows, head)
    nk = new_keys.reshape(owned * steps * kv, head)
    nv = new_values.reshape(owned * steps * kv, head)
    keys = key_pool.reshape(slots, block_len * kv, head)
    values = value_pool.reshape(slots, block_len * kv, head)

    def ask(turn):
        message = pl.pallas_call(
            functools.partial(request_kernel, owned, rows, block_len),
            out_shape=jax.ShapeDtypeStruct((sources, rows + 16, head), BF16),
            in_specs=[smem(), smem(), smem(), vmem()],
            out_specs=vmem(),
            scratch_shapes=[pltpu.SMEM((owned,), jnp.int32)],
            name="ask",
        )(turn, slot_block, lengths, q)
        return lax.all_to_all(message, "ctx", split_axis=0, concat_axis=0, tiled=True)

    def buffers(sets):
        return [
            pltpu.VMEM((slots, block_len * kv, head), BF16),
            pltpu.VMEM((slots, block_len * kv, head), BF16),
            pltpu.SemaphoreType.DMA((slots,)),
            pltpu.SemaphoreType.DMA((slots,)),
            pltpu.SMEM((slots,), jnp.int32),
            pltpu.VMEM((sets, rows, 128), F32),
            pltpu.VMEM((sets, rows, 128), F32),
            pltpu.VMEM((sets, rows, head), F32),
        ]

    got = ask(jnp.zeros((1,), jnp.int32))
    own, lse = pl.pallas_call(
        functools.partial(own_kernel, owned, steps, kv, group),
        out_shape=(
            jax.ShapeDtypeStruct((owned, rows, head), BF16),
            jax.ShapeDtypeStruct((rows, 128), F32),
        ),
        in_specs=[smem(), smem(), vmem(), vmem(), vmem(), hbm(), hbm()],
        out_specs=(vmem(), vmem()),
        scratch_shapes=buffers(owned),
        name="own",
        compiler_params=pltpu.CompilerParams(vmem_limit_bytes=40 * 2**20),
    )(slot_block, lengths, q, nk, nv, keys, values)

    rounds = jnp.max(got[:, rows, 0]).astype(jnp.int32)
    here = lax.axis_index("ctx")
    request = slot_block // MAXB
    lent = (slot_block >= 0) & (request // owned != here)
    wanted = jnp.max(jnp.where(lent, request % owned, -1)).astype(F32)

    def more(state):
        return state[0] < rounds

    def next_round(state):
        turn, held = state
        fresh = ask(turn.reshape(1))
        match = fresh[:, rows + 1, 0].astype(F32) == wanted
        return turn + 1, jnp.where(match[:, None, None], fresh, held)

    _, got = lax.while_loop(more, next_round, (jnp.int32(1), got))

    partial = pl.pallas_call(
        functools.partial(lent_kernel, owned, kv, group),
        out_shape=jax.ShapeDtypeStruct((2, rows, head), BF16),
        in_specs=[smem(), smem(), vmem(), vmem(), hbm(), hbm()],
        out_specs=vmem(),
        scratch_shapes=buffers(1),
        name="lent",
        compiler_params=pltpu.CompilerParams(vmem_limit_bytes=40 * 2**20),
    )(slot_block, lengths, got, lse, keys, values)

    pieces = [own]
    for d in range(1, sources):
        bit = 1 if d % 2 else d
        pieces.append(
            lax.ppermute(pieces[d ^ bit], "ctx", [(i, i ^ bit) for i in range(sources)])
        )
    spread = lax.all_to_all(
        jnp.broadcast_to(partial[None], (sources,) + partial.shape),
        "ctx", split_axis=0, concat_axis=0, tiled=True,
    )
    count = sources * owned * steps
    kept = count // parts
    send, keep = pl.pallas_call(
        functools.partial(project_kernel, owned, steps, heads, sources, parts),
        out_shape=(
            jax.ShapeDtypeStruct((parts // 2, kept, cols), BF16),
            jax.ShapeDtypeStruct((parts // 2, kept, cols), BF16),
        ),
        in_specs=[vmem()] * (1 + sources) + [hbm()],
        out_specs=(vmem(), vmem()),
        scratch_shapes=[
            pltpu.VMEM((sources * owned * rows, head), F32),
            pltpu.VMEM((sources, rows, 128), F32),
            pltpu.VMEM((count, heads * head), BF16),
            pltpu.VMEM(out_weight.shape, BF16),
            pltpu.SemaphoreType.DMA,
        ],
        name="project",
        compiler_params=pltpu.CompilerParams(vmem_limit_bytes=48 * 2**20),
    )(spread, *pieces, out_weight)

    bit = 1
    while True:
        other = lax.ppermute(send, "tp", [(i, i ^ bit) for i in range(parts)])
        held = keep.astype(F32) + other.astype(F32)
        bit *= 2
        if bit == parts:
            break
        held = held.reshape((held.shape[0] // 2, 2) + held.shape[1:])
        send, keep = held[:, 1].astype(BF16), held[:, 0]
    return held.astype(BF16).reshape(kept // steps, steps, cols)


def solution(mesh):
    return jax.shard_map(
        per_device,
        mesh=mesh,
        in_specs=(
            P("ctx", None, "tp", None),
            P("ctx", None, "tp", None),
            P("ctx", None, "tp", None),
            P("ctx", None, "tp", None),
            P("ctx", None, "tp", None),
            P("ctx"),
            P(),
            P("tp", "ctx"),
        ),
        out_specs=P("tp", None, "ctx"),
        check_vma=False,
    )
```

```python
import functools
import math

import jax
import jax.numpy as jnp
from jax import lax
from jax.experimental import pallas as pl
from jax.experimental.pallas import tpu as pltpu
from jax.sharding import PartitionSpec as P

MAXB = 128
GROUP = 4
AHEAD = 16
COST = 10**10
NEG = -1e30
LOG2E = math.log2(math.e)
F32 = jnp.float32
BF16 = jnp.bfloat16

NT = (((1,), (1,)), ((), ()))


def request_kernel(owned, rows, block_len, round_ref, slot_ref, len_ref, q_ref, out_ref, count):
    me = lax.axis_index("ctx")
    for r in range(owned):
        count[r] = 0

    shift = MAXB.bit_length() - 1

    def tally(s, carry):
        local = lax.shift_right_arithmetic(slot_ref[s], shift) - me * owned
        local = jnp.where((local >= 0) & (local < owned), local, owned)
        count[local] = count[local] + 1
        return carry

    lax.fori_loop(0, slot_ref.shape[0], tally, 0, unroll=8)
    seen = jnp.int32(0)
    pick = jnp.int32(-1)
    for r in range(owned):
        blocks = lax.div(len_ref[me * owned + r] + (block_len - 1), block_len)
        lent = count[r] < blocks
        pick = jnp.where(lent & (seen == round_ref[0]), r, pick)
        seen = seen + lent.astype(jnp.int32)
    row = lax.broadcasted_iota(jnp.int32, (16, 128), 0)
    info = jnp.where(row == 0, seen, pick).astype(F32).astype(BF16)
    body = q_ref[jnp.maximum(pick, 0)]
    for c in range(out_ref.shape[0]):
        out_ref[c, pl.ds(0, rows), :] = body
        out_ref[c, pl.ds(rows, 16), :] = info


def attend(
    foreign, owned, kv, group, slot_ref, len_ref, query_of, first,
    k_hbm, v_hbm, kbuf, vbuf, ksem, vsem, order, sbuf, hbuf, m_acc, l_acc, a_acc,
):
    me = lax.axis_index("ctx")
    width, head = kbuf.shape[1:]
    block_len = width // kv
    rows = m_acc.shape[1]
    heads = group * kv
    coef = head ** -0.5 * LOG2E
    shift = MAXB.bit_length() - 1
    low, past = me * owned, (me + 1) * owned

    def begin(s, n):
        code = slot_ref[s]
        r = lax.shift_right_arithmetic(code, shift)
        inside = (r >= low) & (r < past)
        mine = (code >= 0) & (jnp.logical_not(inside) if foreign else inside)
        order[n] = s
        return n + mine.astype(jnp.int32)

    n = lax.fori_loop(0, slot_ref.shape[0], begin, jnp.int32(0), unroll=8)

    def fetch(i, carry):
        s = order[i]
        pltpu.make_async_copy(k_hbm.at[s], kbuf.at[i], ksem.at[i]).start()
        pltpu.make_async_copy(v_hbm.at[s], vbuf.at[i], vsem.at[i]).start()
        return carry

    lax.fori_loop(0, jnp.minimum(n, AHEAD), fetch, 0)
    first()
    col = lax.broadcasted_iota(jnp.int32, (2 * rows, width), 1)
    row = lax.broadcasted_iota(jnp.int32, (2 * rows, width), 0)
    same = (col % kv) == (row % heads) // group
    place = jnp.where(same, col, width * 2)
    none = jnp.zeros((rows, head), BF16)

    def at(i):
        slot = jnp.minimum(i, n - 1)
        code = slot_ref[order[slot]]
        r = lax.shift_right_arithmetic(code, shift)
        valid = jnp.clip(len_ref[r] - (code - r * MAXB) * block_len, 0, block_len)
        valid = jnp.where(i < n, valid, 0) * kv
        return slot, (jnp.int32(0) if foreign else r - low), valid

    def wait(base, source, buf, sem):
        for g in range(GROUP):
            i = base + g

            @pl.when(i < n)
            def _():
                pltpu.make_async_copy(source.at[0], buf.at[i], sem.at[i]).wait()

    def score(base, side):
        for p in range(GROUP // 2):
            sa, ea, va = at(base + 2 * p)
            sb, eb, vb = at(base + 2 * p + 1)
            left = jnp.concatenate(
                [
                    jnp.concatenate([query_of(ea), none], axis=1),
                    jnp.concatenate([none, query_of(eb)], axis=1),
                ],
                axis=0,
            )
            right = jnp.concatenate([kbuf[sa], kbuf[sb]], axis=1)
            raw = lax.dot_general(left, right, NT, preferred_element_type=F32)
            for half, valid in ((0, va), (1, vb)):
                part = slice(half * rows, (half + 1) * rows)
                masked = jnp.where(place[part] < valid, raw[part], NEG)
                sbuf[side, p, part, :] = masked
                high = jnp.max(masked, axis=1, keepdims=True)
                hbuf[side, p, part, :] = jnp.broadcast_to(high, (rows, 128))

    def mix(base, side):
        for p in range(GROUP // 2):
            sa, ea, _ = at(base + 2 * p)
            sb, eb, _ = at(base + 2 * p + 1)
            high = hbuf[side, p]
            total = None
            pieces = []
            for c in range(width // 128):
                w = jnp.exp2((sbuf[side, p, :, c * 128 : (c + 1) * 128] - high) * coef).astype(BF16)
                pieces.append(w)
                rounded = w.astype(F32)
                total = rounded if total is None else total + rounded
            weights = jnp.concatenate(pieces, axis=1)
            right = jnp.concatenate([vbuf[sa], vbuf[sb]], axis=1)
            summed = jnp.dot(weights, right, preferred_element_type=F32)
            for half, e in ((0, ea), (1, eb)):
                part = slice(half * rows, (half + 1) * rows)
                before = m_acc[e]
                peak = jnp.maximum(before, high[part])
                keep = jnp.exp2((before - peak) * coef)
                add = jnp.exp2((high[part] - peak) * coef)
                m_acc[e] = peak
                l_acc[e] = l_acc[e] * keep + total[part] * add
                a_acc[e] = a_acc[e] * keep + summed[part, half * head : (half + 1) * head] * add

    def step(it, carry):
        base = it * GROUP
        lax.fori_loop(jnp.minimum(base + AHEAD, n), jnp.minimum(base + GROUP + AHEAD, n), fetch, 0)
        wait(base + GROUP, k_hbm, kbuf, ksem)
        wait(base, v_hbm, vbuf, vsem)
        side = lax.rem(it, 2)
        score(base + GROUP, 1 - side)
        mix(base, side)
        return carry

    @pl.when(n > 0)
    def _():
        wait(0, k_hbm, kbuf, ksem)
        score(0, 0)
        lax.fori_loop(0, lax.div(n + GROUP - 1, GROUP), step, 0)


def own_kernel(
    owned, steps, kv, group, slot_ref, len_ref, q_ref, nk_hbm, nv_hbm, k_hbm, v_hbm,
    out_ref, lse_ref, nk_ref, nv_ref, nsem, kbuf, vbuf, ksem, vsem, order, sbuf, hbuf, m_acc, l_acc, a_acc,
):
    rows, head = q_ref.shape[1:]
    heads = kv * group
    coef = head ** -0.5 * LOG2E
    fresh = nk_ref.shape[0]
    nk_copy = pltpu.make_async_copy(nk_hbm, nk_ref, nsem.at[0])
    nv_copy = pltpu.make_async_copy(nv_hbm, nv_ref, nsem.at[1])
    nk_copy.start()
    nv_copy.start()
    col = lax.broadcasted_iota(jnp.int32, (rows, fresh), 1)
    row = lax.broadcasted_iota(jnp.int32, (rows, fresh), 0)
    seen = ((col % kv) == (row % heads) // group) & (lax.div(col, kv) % steps <= lax.div(row, heads))
    lane = lax.broadcasted_iota(jnp.int32, (rows, 128), 1)

    def first():
        nk_copy.wait()
        nv_copy.wait()
        nk = nk_ref[...]
        nv = nv_ref[...]
        for r in range(owned):
            scores = lax.dot_general(q_ref[r], nk, NT, preferred_element_type=F32)
            ok = seen & (lax.div(col, kv * steps) == r)
            scores = jnp.where(ok, scores, NEG)
            high = jnp.max(scores, axis=1, keepdims=True)
            weights = jnp.where(ok, jnp.exp2((scores - high) * coef), 0.0).astype(BF16)
            total = jnp.sum(weights.astype(F32), axis=1, keepdims=True)
            m_acc[r] = jnp.broadcast_to(high, (rows, 128))
            l_acc[r] = jnp.where(lane == 0, total, 0.0)
            a_acc[r] = jnp.dot(weights, nv, preferred_element_type=F32)

    attend(
        False, owned, kv, group, slot_ref, len_ref, lambda e: q_ref[e], first,
        k_hbm, v_hbm, kbuf, vbuf, ksem, vsem, order, sbuf, hbuf, m_acc, l_acc, a_acc,
    )
    table = jnp.zeros((rows, 128), F32)
    for r in range(owned):
        total = jnp.sum(l_acc[r], axis=1, keepdims=True)
        out_ref[r] = (a_acc[r] / total).astype(BF16)
        table = jnp.where(lane % 32 == r, m_acc[r] * coef + jnp.log(total) * LOG2E, table)
    lse_ref[...] = table


def lent_kernel(
    owned, kv, group, slot_ref, len_ref, got_ref, own_ref, lse_ref, k_hbm, v_hbm,
    out_ref, info_ref, kbuf, vbuf, ksem, vsem, order, sbuf, hbuf, m_acc, l_acc, a_acc,
):
    rows, head = out_ref.shape[1:]
    coef = head ** -0.5 * LOG2E
    me = lax.axis_index("ctx")

    shift = MAXB.bit_length() - 1

    def find(s, rid):
        code = slot_ref[s]
        r = lax.shift_right_arithmetic(code, shift)
        inside = (r >= me * owned) & (r < (me + 1) * owned)
        return jnp.where((code >= 0) & jnp.logical_not(inside), r, rid)

    rid = lax.fori_loop(0, slot_ref.shape[0], find, jnp.int32(0), unroll=8)
    owner = lax.div(rid, owned)
    most = got_ref[0, pl.ds(rows, 16), :].astype(F32)
    for c in range(1, got_ref.shape[0]):
        most = jnp.maximum(most, got_ref[c, pl.ds(rows, 16), :].astype(F32))
    info_ref[0] = jnp.max(most[:1]).astype(jnp.int32)
    sent = jnp.max(got_ref[owner, pl.ds(rows, 16), :].astype(F32)[1:2]).astype(jnp.int32)
    info_ref[1] = (sent == lax.rem(rid, owned)).astype(jnp.int32)

    def first():
        m_acc[0] = jnp.full((rows, 128), NEG, F32)
        l_acc[0] = jnp.zeros((rows, 128), F32)
        a_acc[0] = jnp.zeros((rows, head), F32)
        out_ref[pl.ds(0, owned)] = own_ref[...]

    attend(
        True, owned, kv, group, slot_ref, len_ref, lambda e: got_ref[owner, pl.ds(0, rows), :], first,
        k_hbm, v_hbm, kbuf, vbuf, ksem, vsem, order, sbuf, hbuf, m_acc, l_acc, a_acc,
    )
    total = jnp.sum(l_acc[0], axis=1, keepdims=True)
    some = total > 0.0
    total = jnp.where(some, total, 1.0)
    out_ref[owned] = (a_acc[0] / total).astype(BF16)
    lse = jnp.where(some, m_acc[0] * coef + jnp.log(total) * LOG2E, NEG)
    lane = lax.broadcasted_iota(jnp.int32, (rows, 128), 1)
    table = jnp.where(lane % 32 == owned, lse, lse_ref[...])
    table = jnp.where(lane % 32 == owned + 1, rid.astype(F32), table)
    second = table - table.astype(BF16).astype(F32)
    third = second - second.astype(BF16).astype(F32)
    out_ref[owned + 1] = jnp.where(lane < 32, table, jnp.where(lane < 64, second, third)).astype(BF16)


def project_kernel(
    owned, steps, heads, sources, parts, *refs
):
    pieces = refs[:sources]
    w_hbm, send_ref, keep_ref, full, lse, flat, wbuf, wsem = refs[sources:]
    me = lax.axis_index("ctx")
    mine = lax.axis_index("tp")
    rows = steps * heads
    head = full.shape[1]
    span = owned * rows
    per = sources // parts
    copy = pltpu.make_async_copy(w_hbm, wbuf, wsem)
    copy.start()

    def spot(c):
        return (lax.div(c, per) ^ mine) * per + lax.rem(c, per)

    lane = lax.broadcasted_iota(jnp.int32, (rows, 128), 1)
    for d in range(sources):
        start = pl.multiple_of(spot(me ^ d) * span, span)
        full[pl.ds(start, span), :] = pieces[d][pl.ds(0, owned)].astype(F32).reshape(span, head)
    rids = []
    theirs = []
    for d in range(sources):
        packed = pieces[d][owned + 1].astype(F32)
        table = packed + pltpu.roll(packed, 96, 1) + pltpu.roll(packed, 64, 1)
        lse[me ^ d] = table
        theirs.append(jnp.sum(jnp.where(lane == owned, table, 0.0), axis=1, keepdims=True))
        rids.append(jnp.max(jnp.where(lane[:8] == owned + 1, table[:8], -1.0)).astype(jnp.int32))
    for d in range(sources):
        c = lax.div(rids[d], owned)
        r = lax.rem(rids[d], owned)
        start = pl.multiple_of((spot(c) * owned + r) * rows, rows)
        table = lse[c]
        left = jnp.sum(jnp.where(lane == r, table, 0.0), axis=1, keepdims=True)
        right = theirs[d]
        peak = jnp.maximum(left, right)
        w_left = jnp.exp2(left - peak)
        w_right = jnp.exp2(right - peak)
        total = w_left + w_right
        full[pl.ds(start, rows), :] = full[pl.ds(start, rows), :] * (w_left / total) + pieces[
            d
        ][owned].astype(F32) * (w_right / total)
        lse[c] = jnp.where(lane == r, peak + jnp.log(total) * LOG2E, table)
    count = sources * owned * steps
    for h in range(heads):
        flat[:, h * head : (h + 1) * head] = full[pl.ds(h, count, stride=heads), :].astype(BF16)
    copy.wait()
    result = jnp.dot(flat[...], wbuf[...], preferred_element_type=F32).astype(BF16)
    kept = count // parts
    for b in range(parts):
        target = keep_ref if b % 2 == 0 else send_ref
        target[b // 2] = result[b * kept : (b + 1) * kept]


def smem():
    return pl.BlockSpec(memory_space=pltpu.SMEM)


def vmem():
    return pl.BlockSpec(memory_space=pltpu.VMEM)


def hbm():
    return pl.BlockSpec(memory_space=pltpu.HBM)


def in_hbm(x):
    return pltpu.with_memory_space_constraint(x, pltpu.HBM)


def per_device(
    queries, new_keys, new_values, key_pool, value_pool, slot_block, lengths, out_weight
):
    owned, steps, heads, head = queries.shape
    kv = new_keys.shape[2]
    group = heads // kv
    slots, block_len = key_pool.shape[:2]
    sources = lax.axis_size("ctx")
    parts = lax.axis_size("tp")
    rows = steps * heads
    cols = out_weight.shape[1]
    q = queries.reshape(owned, rows, head)
    nk = in_hbm(new_keys.reshape(owned * steps * kv, head))
    nv = in_hbm(new_values.reshape(owned * steps * kv, head))
    keys = in_hbm(key_pool.reshape(slots, block_len * kv, head))
    values = in_hbm(value_pool.reshape(slots, block_len * kv, head))
    weight = in_hbm(out_weight)

    def ask(turn):
        message = pl.pallas_call(
            functools.partial(request_kernel, owned, rows, block_len),
            out_shape=jax.ShapeDtypeStruct((sources, rows + 16, head), BF16),
            in_specs=[smem(), smem(), smem(), vmem()],
            out_specs=vmem(),
            scratch_shapes=[pltpu.SMEM((owned + 1,), jnp.int32)],
            name="ask",
        )(turn, slot_block, lengths, q)
        return lax.all_to_all(message, "ctx", split_axis=0, concat_axis=0, tiled=True)

    cost = pl.CostEstimate(flops=COST, bytes_accessed=key_pool.size * 4, transcendentals=0)

    def buffers(sets):
        return [
            pltpu.VMEM((slots, block_len * kv, head), BF16),
            pltpu.VMEM((slots, block_len * kv, head), BF16),
            pltpu.SemaphoreType.DMA((slots,)),
            pltpu.SemaphoreType.DMA((slots,)),
            pltpu.SMEM((slots + 1,), jnp.int32),
            pltpu.VMEM((2, GROUP // 2, 2 * rows, block_len * kv), F32),
            pltpu.VMEM((2, GROUP // 2, 2 * rows, 128), F32),
            pltpu.VMEM((sets, rows, 128), F32),
            pltpu.VMEM((sets, rows, 128), F32),
            pltpu.VMEM((sets, rows, head), F32),
        ]

    got = ask(jnp.zeros((1,), jnp.int32))
    own, lse = pl.pallas_call(
        functools.partial(own_kernel, owned, steps, kv, group),
        out_shape=(
            jax.ShapeDtypeStruct((owned, rows, head), BF16),
            jax.ShapeDtypeStruct((rows, 128), F32),
        ),
        in_specs=[smem(), smem(), vmem(), hbm(), hbm(), hbm(), hbm()],
        out_specs=(vmem(), vmem()),
        scratch_shapes=[
            pltpu.VMEM(nk.shape, BF16),
            pltpu.VMEM(nv.shape, BF16),
            pltpu.SemaphoreType.DMA((2,)),
        ]
        + buffers(owned),
        cost_estimate=cost,
        name="own",
        compiler_params=pltpu.CompilerParams(vmem_limit_bytes=40 * 2**20),
    )(slot_block, lengths, q, nk, nv, keys, values)

    def answer(got):
        return pl.pallas_call(
            functools.partial(lent_kernel, owned, kv, group),
            out_shape=(
                jax.ShapeDtypeStruct((owned + 2, rows, head), BF16),
                jax.ShapeDtypeStruct((2,), jnp.int32),
            ),
            in_specs=[smem(), smem(), vmem(), vmem(), vmem(), hbm(), hbm()],
            out_specs=(vmem(), smem()),
            scratch_shapes=buffers(1),
            cost_estimate=cost,
            name="lent",
            compiler_params=pltpu.CompilerParams(vmem_limit_bytes=40 * 2**20),
        )(slot_block, lengths, got, own, lse, keys, values)

    partial, info = answer(got)

    def more(state):
        return state[0] < state[1]

    def next_round(state):
        turn, rounds, held = state
        fresh, info = answer(ask(turn.reshape(1)))
        return turn + 1, rounds, jnp.where(info[1] > 0, fresh, held)

    _, _, partial = lax.while_loop(more, next_round, (jnp.int32(1), info[0], partial))

    pieces = [partial]
    for d in range(1, sources):
        bit = 1 if d % 2 else d
        pieces.append(
            lax.ppermute(pieces[d ^ bit], "ctx", [(i, i ^ bit) for i in range(sources)])
        )
    count = sources * owned * steps
    kept = count // parts
    send, keep = pl.pallas_call(
        functools.partial(project_kernel, owned, steps, heads, sources, parts),
        out_shape=(
            jax.ShapeDtypeStruct((parts // 2, kept, cols), BF16),
            jax.ShapeDtypeStruct((parts // 2, kept, cols), BF16),
        ),
        in_specs=[vmem()] * sources + [hbm()],
        out_specs=(vmem(), vmem()),
        scratch_shapes=[
            pltpu.VMEM((sources * owned * rows, head), F32),
            pltpu.VMEM((sources, rows, 128), F32),
            pltpu.VMEM((count, heads * head), BF16),
            pltpu.VMEM(out_weight.shape, BF16),
            pltpu.SemaphoreType.DMA,
        ],
        name="project",
        compiler_params=pltpu.CompilerParams(vmem_limit_bytes=48 * 2**20),
    )(*pieces, weight)

    bit = 1
    while True:
        other = lax.ppermute(send, "tp", [(i, i ^ bit) for i in range(parts)])
        held = keep.astype(F32) + other.astype(F32)
        bit *= 2
        if bit == parts:
            break
        held = held.reshape((held.shape[0] // 2, 2) + held.shape[1:])
        send, keep = held[:, 1].astype(BF16), held[:, 0]
    return held.astype(BF16).reshape(kept // steps, steps, cols)


def solution(mesh):
    return jax.shard_map(
        per_device,
        mesh=mesh,
        in_specs=(
            P("ctx", None, "tp", None),
            P("ctx", None, "tp", None),
            P("ctx", None, "tp", None),
            P("ctx", None, "tp", None),
            P("ctx", None, "tp", None),
            P("ctx"),
            P(),
            P("tp", "ctx"),
        ),
        out_specs=P("tp", None, "ctx"),
        check_vma=False,
    )
```

```python
import functools
import math

import jax
import jax.numpy as jnp
from jax import lax
from jax.experimental import pallas as pl
from jax.experimental.pallas import tpu as pltpu
from jax.sharding import PartitionSpec as P


MAXB = 128
GROUP = 8
AHEAD = 32
COST = 10**10
NEG = -1e30
LOG2E = math.log2(math.e)
F32 = jnp.float32
BF16 = jnp.bfloat16

NT = (((1,), (1,)), ((), ()))


def request_kernel(owned, rows, block_len, round_ref, slot_ref, len_ref, q_ref, out_ref, count):
    me = lax.axis_index("ctx")
    for r in range(owned):
        count[r] = 0

    shift = MAXB.bit_length() - 1

    def tally(s, carry):
        local = lax.shift_right_arithmetic(slot_ref[s], shift) - me * owned
        local = jnp.where((local >= 0) & (local < owned), local, owned)
        count[local] = count[local] + 1
        return carry

    lax.fori_loop(0, slot_ref.shape[0], tally, 0, unroll=8)
    seen = jnp.int32(0)
    pick = jnp.int32(-1)
    for r in range(owned):
        blocks = lax.div(len_ref[me * owned + r] + (block_len - 1), block_len)
        lent = count[r] < blocks
        pick = jnp.where(lent & (seen == round_ref[0]), r, pick)
        seen = seen + lent.astype(jnp.int32)
    row = lax.broadcasted_iota(jnp.int32, (16, 128), 0)
    info = jnp.where(row == 0, seen, pick).astype(F32).astype(BF16)
    body = q_ref[jnp.maximum(pick, 0)]
    for c in range(out_ref.shape[0]):
        out_ref[c, pl.ds(0, rows), :] = body
        out_ref[c, pl.ds(rows, 16), :] = info


def attend(
    foreign, owned, kv, group, slot_ref, len_ref, query_of, first,
    k_hbm, v_hbm, kbuf, vbuf, ksem, vsem, order, sbuf, hbuf, m_acc, l_acc, a_acc,
):
    me = lax.axis_index("ctx")
    width, head = kbuf.shape[1:]
    block_len = width // kv
    rows = m_acc.shape[1]
    heads = group * kv
    coef = head ** -0.5 * LOG2E
    shift = MAXB.bit_length() - 1
    low, past = me * owned, (me + 1) * owned

    def begin(s, n):
        code = slot_ref[s]
        r = lax.shift_right_arithmetic(code, shift)
        inside = (r >= low) & (r < past)
        mine = (code >= 0) & (jnp.logical_not(inside) if foreign else inside)
        order[n] = s
        return n + mine.astype(jnp.int32)

    n = lax.fori_loop(0, slot_ref.shape[0], begin, jnp.int32(0), unroll=8)

    def fetch(i, carry):
        s = order[i]
        pltpu.make_async_copy(k_hbm.at[s], kbuf.at[i], ksem.at[i]).start()
        pltpu.make_async_copy(v_hbm.at[s], vbuf.at[i], vsem.at[i]).start()
        return carry

    lax.fori_loop(0, jnp.minimum(n, AHEAD), fetch, 0)
    first()
    col = lax.broadcasted_iota(jnp.int32, (2 * rows, width), 1)
    row = lax.broadcasted_iota(jnp.int32, (2 * rows, width), 0)
    same = (col % kv) == (row % heads) // group
    place = jnp.where(same, col, width * 2)
    none = jnp.zeros((rows, head), BF16)

    def at(i):
        slot = jnp.minimum(i, n - 1)
        code = slot_ref[order[slot]]
        r = lax.shift_right_arithmetic(code, shift)
        valid = jnp.clip(len_ref[r] - (code - r * MAXB) * block_len, 0, block_len)
        valid = jnp.where(i < n, valid, 0) * kv
        return slot, (jnp.int32(0) if foreign else r - low), valid

    def wait(base, source, buf, sem):
        for g in range(GROUP):
            i = base + g

            @pl.when(i < n)
            def _():
                pltpu.make_async_copy(source.at[0], buf.at[i], sem.at[i]).wait()

    def score(base, side):
        for p in range(GROUP // 2):
            sa, ea, va = at(base + 2 * p)
            sb, eb, vb = at(base + 2 * p + 1)
            left = jnp.concatenate(
                [
                    jnp.concatenate([query_of(ea), none], axis=1),
                    jnp.concatenate([none, query_of(eb)], axis=1),
                ],
                axis=0,
            )
            right = jnp.concatenate([kbuf[sa], kbuf[sb]], axis=1)
            raw = lax.dot_general(left, right, NT, preferred_element_type=F32)
            for half, valid in ((0, va), (1, vb)):
                part = slice(half * rows, (half + 1) * rows)
                masked = jnp.where(place[part] < valid, raw[part], NEG)
                sbuf[side, p, part, :] = masked
                high = jnp.max(masked, axis=1, keepdims=True)
                hbuf[side, p, part, :] = jnp.broadcast_to(high, (rows, 128))

    def mix(base, side):
        for p in range(GROUP // 2):
            sa, ea, _ = at(base + 2 * p)
            sb, eb, _ = at(base + 2 * p + 1)
            high = hbuf[side, p]
            total = None
            pieces = []
            for c in range(width // 128):
                w = jnp.exp2((sbuf[side, p, :, c * 128 : (c + 1) * 128] - high) * coef).astype(BF16)
                pieces.append(w)
                rounded = w.astype(F32)
                total = rounded if total is None else total + rounded
            weights = jnp.concatenate(pieces, axis=1)
            right = jnp.concatenate([vbuf[sa], vbuf[sb]], axis=1)
            summed = jnp.dot(weights, right, preferred_element_type=F32)
            for half, e in ((0, ea), (1, eb)):
                part = slice(half * rows, (half + 1) * rows)
                before = m_acc[e]
                peak = jnp.maximum(before, high[part])
                keep = jnp.exp2((before - peak) * coef)
                add = jnp.exp2((high[part] - peak) * coef)
                m_acc[e] = peak
                l_acc[e] = l_acc[e] * keep + total[part] * add
                a_acc[e] = a_acc[e] * keep + summed[part, half * head : (half + 1) * head] * add

    def step(it, carry):
        base = it * GROUP
        lax.fori_loop(jnp.minimum(base + AHEAD, n), jnp.minimum(base + GROUP + AHEAD, n), fetch, 0)
        wait(base + GROUP, k_hbm, kbuf, ksem)
        wait(base, v_hbm, vbuf, vsem)
        side = lax.rem(it, 2)
        score(base + GROUP, 1 - side)
        mix(base, side)
        return carry

    @pl.when(n > 0)
    def _():
        wait(0, k_hbm, kbuf, ksem)
        score(0, 0)
        lax.fori_loop(0, lax.div(n + GROUP - 1, GROUP), step, 0)


def own_kernel(
    owned, steps, kv, group, slot_ref, len_ref, q_ref, nk_hbm, nv_hbm, k_hbm, v_hbm,
    out_ref, lse_ref, nk_ref, nv_ref, nsem, kbuf, vbuf, ksem, vsem, order, sbuf, hbuf, m_acc, l_acc, a_acc,
):
    rows, head = q_ref.shape[1:]
    heads = kv * group
    coef = head ** -0.5 * LOG2E
    fresh = nk_ref.shape[0]
    nk_copy = pltpu.make_async_copy(nk_hbm, nk_ref, nsem.at[0])
    nv_copy = pltpu.make_async_copy(nv_hbm, nv_ref, nsem.at[1])
    nk_copy.start()
    nv_copy.start()
    col = lax.broadcasted_iota(jnp.int32, (rows, fresh), 1)
    row = lax.broadcasted_iota(jnp.int32, (rows, fresh), 0)
    seen = ((col % kv) == (row % heads) // group) & (lax.div(col, kv) % steps <= lax.div(row, heads))
    lane = lax.broadcasted_iota(jnp.int32, (rows, 128), 1)

    def first():
        nk_copy.wait()
        nv_copy.wait()
        nk = nk_ref[...]
        nv = nv_ref[...]
        for r in range(owned):
            scores = lax.dot_general(q_ref[r], nk, NT, preferred_element_type=F32)
            ok = seen & (lax.div(col, kv * steps) == r)
            scores = jnp.where(ok, scores, NEG)
            high = jnp.max(scores, axis=1, keepdims=True)
            weights = jnp.where(ok, jnp.exp2((scores - high) * coef), 0.0).astype(BF16)
            total = jnp.sum(weights.astype(F32), axis=1, keepdims=True)
            m_acc[r] = jnp.broadcast_to(high, (rows, 128))
            l_acc[r] = jnp.where(lane == 0, total, 0.0)
            a_acc[r] = jnp.dot(weights, nv, preferred_element_type=F32)

    attend(
        False, owned, kv, group, slot_ref, len_ref, lambda e: q_ref[e], first,
        k_hbm, v_hbm, kbuf, vbuf, ksem, vsem, order, sbuf, hbuf, m_acc, l_acc, a_acc,
    )
    table = jnp.zeros((rows, 128), F32)
    for r in range(owned):
        total = jnp.sum(l_acc[r], axis=1, keepdims=True)
        out_ref[r] = (a_acc[r] / total).astype(BF16)
        table = jnp.where(lane % 32 == r, m_acc[r] * coef + jnp.log(total) * LOG2E, table)
    lse_ref[...] = table


def lent_kernel(
    owned, kv, group, slot_ref, len_ref, got_ref, own_ref, lse_ref, k_hbm, v_hbm,
    out_ref, info_ref, kbuf, vbuf, ksem, vsem, order, sbuf, hbuf, m_acc, l_acc, a_acc,
):
    rows, head = out_ref.shape[1:]
    coef = head ** -0.5 * LOG2E
    me = lax.axis_index("ctx")

    shift = MAXB.bit_length() - 1

    def find(s, rid):
        code = slot_ref[s]
        r = lax.shift_right_arithmetic(code, shift)
        inside = (r >= me * owned) & (r < (me + 1) * owned)
        return jnp.where((code >= 0) & jnp.logical_not(inside), r, rid)

    rid = lax.fori_loop(0, slot_ref.shape[0], find, jnp.int32(0), unroll=8)
    owner = lax.div(rid, owned)
    most = got_ref[0, pl.ds(rows, 16), :].astype(F32)
    for c in range(1, got_ref.shape[0]):
        most = jnp.maximum(most, got_ref[c, pl.ds(rows, 16), :].astype(F32))
    info_ref[0] = jnp.max(most[:1]).astype(jnp.int32)
    sent = jnp.max(got_ref[owner, pl.ds(rows, 16), :].astype(F32)[1:2]).astype(jnp.int32)
    info_ref[1] = (sent == lax.rem(rid, owned)).astype(jnp.int32)

    def first():
        m_acc[0] = jnp.full((rows, 128), NEG, F32)
        l_acc[0] = jnp.zeros((rows, 128), F32)
        a_acc[0] = jnp.zeros((rows, head), F32)
        out_ref[pl.ds(0, owned)] = own_ref[...]

    attend(
        True, owned, kv, group, slot_ref, len_ref, lambda e: got_ref[owner, pl.ds(0, rows), :], first,
        k_hbm, v_hbm, kbuf, vbuf, ksem, vsem, order, sbuf, hbuf, m_acc, l_acc, a_acc,
    )
    total = jnp.sum(l_acc[0], axis=1, keepdims=True)
    some = total > 0.0
    total = jnp.where(some, total, 1.0)
    out_ref[owned] = (a_acc[0] / total).astype(BF16)
    lse = jnp.where(some, m_acc[0] * coef + jnp.log(total) * LOG2E, NEG)
    lane = lax.broadcasted_iota(jnp.int32, (rows, 128), 1)
    table = jnp.where(lane % 32 == owned, lse, lse_ref[...])
    table = jnp.where(lane % 32 == owned + 1, rid.astype(F32), table)
    second = table - table.astype(BF16).astype(F32)
    third = second - second.astype(BF16).astype(F32)
    out_ref[owned + 1] = jnp.where(lane < 32, table, jnp.where(lane < 64, second, third)).astype(BF16)


def project_kernel(
    owned, steps, heads, sources, parts, *refs
):
    pieces = refs[:sources]
    w_hbm, send_ref, keep_ref, full, lse, flat, wbuf, wsem = refs[sources:]
    me = lax.axis_index("ctx")
    mine = lax.axis_index("tp")
    rows = steps * heads
    head = full.shape[1]
    span = owned * rows
    per = sources // parts
    copy = pltpu.make_async_copy(w_hbm, wbuf, wsem)
    copy.start()

    def spot(c):
        return (lax.div(c, per) ^ mine) * per + lax.rem(c, per)

    lane = lax.broadcasted_iota(jnp.int32, (rows, 128), 1)
    for d in range(sources):
        start = pl.multiple_of(spot(me ^ d) * span, span)
        full[pl.ds(start, span), :] = pieces[d][pl.ds(0, owned)].astype(F32).reshape(span, head)
    rids = []
    theirs = []
    for d in range(sources):
        packed = pieces[d][owned + 1].astype(F32)
        table = packed + pltpu.roll(packed, 96, 1) + pltpu.roll(packed, 64, 1)
        lse[me ^ d] = table
        theirs.append(jnp.sum(jnp.where(lane == owned, table, 0.0), axis=1, keepdims=True))
        rids.append(jnp.max(jnp.where(lane[:8] == owned + 1, table[:8], -1.0)).astype(jnp.int32))
    for d in range(sources):
        c = lax.div(rids[d], owned)
        r = lax.rem(rids[d], owned)
        start = pl.multiple_of((spot(c) * owned + r) * rows, rows)
        table = lse[c]
        left = jnp.sum(jnp.where(lane == r, table, 0.0), axis=1, keepdims=True)
        right = theirs[d]
        peak = jnp.maximum(left, right)
        w_left = jnp.exp2(left - peak)
        w_right = jnp.exp2(right - peak)
        total = w_left + w_right
        full[pl.ds(start, rows), :] = full[pl.ds(start, rows), :] * (w_left / total) + pieces[
            d
        ][owned].astype(F32) * (w_right / total)
        lse[c] = jnp.where(lane == r, peak + jnp.log(total) * LOG2E, table)
    count = sources * owned * steps
    for h in range(heads):
        flat[:, h * head : (h + 1) * head] = full[pl.ds(h, count, stride=heads), :].astype(BF16)
    copy.wait()
    result = jnp.dot(flat[...], wbuf[...], preferred_element_type=F32).astype(BF16)
    kept = count // parts
    for b in range(parts):
        target = keep_ref if b % 2 == 0 else send_ref
        target[b // 2] = result[b * kept : (b + 1) * kept]


def smem():
    return pl.BlockSpec(memory_space=pltpu.SMEM)


def vmem():
    return pl.BlockSpec(memory_space=pltpu.VMEM)


def hbm():
    return pl.BlockSpec(memory_space=pltpu.HBM)


def in_hbm(x):
    return pltpu.with_memory_space_constraint(x, pltpu.HBM)


def per_device(
    queries, new_keys, new_values, key_pool, value_pool, slot_block, lengths, out_weight
):
    owned, steps, heads, head = queries.shape
    kv = new_keys.shape[2]
    group = heads // kv
    slots, block_len = key_pool.shape[:2]
    sources = lax.axis_size("ctx")
    parts = lax.axis_size("tp")
    rows = steps * heads
    cols = out_weight.shape[1]
    q = queries.reshape(owned, rows, head)
    nk = in_hbm(new_keys.reshape(owned * steps * kv, head))
    nv = in_hbm(new_values.reshape(owned * steps * kv, head))
    keys = in_hbm(key_pool.reshape(slots, block_len * kv, head))
    values = in_hbm(value_pool.reshape(slots, block_len * kv, head))
    weight = in_hbm(out_weight)

    def ask(turn):
        message = pl.pallas_call(
            functools.partial(request_kernel, owned, rows, block_len),
            out_shape=jax.ShapeDtypeStruct((sources, rows + 16, head), BF16),
            in_specs=[smem(), smem(), smem(), vmem()],
            out_specs=vmem(),
            scratch_shapes=[pltpu.SMEM((owned + 1,), jnp.int32)],
            name="ask",
        )(turn, slot_block, lengths, q)
        return lax.all_to_all(message, "ctx", split_axis=0, concat_axis=0, tiled=True)

    cost = pl.CostEstimate(flops=COST, bytes_accessed=key_pool.size * 4, transcendentals=0)

    def buffers(sets):
        return [
            pltpu.VMEM((slots, block_len * kv, head), BF16),
            pltpu.VMEM((slots, block_len * kv, head), BF16),
            pltpu.SemaphoreType.DMA((slots,)),
            pltpu.SemaphoreType.DMA((slots,)),
            pltpu.SMEM((slots + 1,), jnp.int32),
            pltpu.VMEM((2, GROUP // 2, 2 * rows, block_len * kv), F32),
            pltpu.VMEM((2, GROUP // 2, 2 * rows, 128), F32),
            pltpu.VMEM((sets, rows, 128), F32),
            pltpu.VMEM((sets, rows, 128), F32),
            pltpu.VMEM((sets, rows, head), F32),
        ]

    got = ask(jnp.zeros((1,), jnp.int32))
    own, lse = pl.pallas_call(
        functools.partial(own_kernel, owned, steps, kv, group),
        out_shape=(
            jax.ShapeDtypeStruct((owned, rows, head), BF16),
            jax.ShapeDtypeStruct((rows, 128), F32),
        ),
        in_specs=[smem(), smem(), vmem(), hbm(), hbm(), hbm(), hbm()],
        out_specs=(vmem(), vmem()),
        scratch_shapes=[
            pltpu.VMEM(nk.shape, BF16),
            pltpu.VMEM(nv.shape, BF16),
            pltpu.SemaphoreType.DMA((2,)),
        ]
        + buffers(owned),
        cost_estimate=cost,
        name="own",
        compiler_params=pltpu.CompilerParams(vmem_limit_bytes=40 * 2**20),
    )(slot_block, lengths, q, nk, nv, keys, values)

    def answer(got):
        return pl.pallas_call(
            functools.partial(lent_kernel, owned, kv, group),
            out_shape=(
                jax.ShapeDtypeStruct((owned + 2, rows, head), BF16),
                jax.ShapeDtypeStruct((2,), jnp.int32),
            ),
            in_specs=[smem(), smem(), vmem(), vmem(), vmem(), hbm(), hbm()],
            out_specs=(vmem(), smem()),
            scratch_shapes=buffers(1),
            cost_estimate=cost,
            name="lent",
            compiler_params=pltpu.CompilerParams(vmem_limit_bytes=40 * 2**20),
        )(slot_block, lengths, got, own, lse, keys, values)

    partial, info = answer(got)

    def more(state):
        return state[0] < state[1]

    def next_round(state):
        turn, rounds, held = state
        fresh, info = answer(ask(turn.reshape(1)))
        return turn + 1, rounds, jnp.where(info[1] > 0, fresh, held)

    _, _, partial = lax.while_loop(more, next_round, (jnp.int32(1), info[0], partial))

    pieces = [partial]
    for d in range(1, sources):
        bit = d & -d
        pieces.append(lax.ppermute(pieces[d ^ bit], "ctx", [(i, i ^ bit) for i in range(sources)]))
    count = sources * owned * steps
    kept = count // parts
    send, keep = pl.pallas_call(
        functools.partial(project_kernel, owned, steps, heads, sources, parts),
        out_shape=(
            jax.ShapeDtypeStruct((parts // 2, kept, cols), BF16),
            jax.ShapeDtypeStruct((parts // 2, kept, cols), BF16),
        ),
        in_specs=[vmem()] * sources + [hbm()],
        out_specs=(vmem(), vmem()),
        scratch_shapes=[
            pltpu.VMEM((sources * owned * rows, head), F32),
            pltpu.VMEM((sources, rows, 128), F32),
            pltpu.VMEM((count, heads * head), BF16),
            pltpu.VMEM(out_weight.shape, BF16),
            pltpu.SemaphoreType.DMA,
        ],
        name="project",
        compiler_params=pltpu.CompilerParams(vmem_limit_bytes=48 * 2**20),
    )(*pieces, weight)

    bit = 1
    while True:
        other = lax.ppermute(send, "tp", [(i, i ^ bit) for i in range(parts)])
        held = keep.astype(F32) + other.astype(F32)
        bit *= 2
        if bit == parts:
            break
        held = held.reshape((held.shape[0] // 2, 2) + held.shape[1:])
        send, keep = held[:, 1].astype(BF16), held[:, 0]
    return held.astype(BF16).reshape(kept // steps, steps, cols)


def solution(mesh):
    return jax.shard_map(
        per_device,
        mesh=mesh,
        in_specs=(
            P("ctx", None, "tp", None),
            P("ctx", None, "tp", None),
            P("ctx", None, "tp", None),
            P("ctx", None, "tp", None),
            P("ctx", None, "tp", None),
            P("ctx"),
            P(),
            P("tp", "ctx"),
        ),
        out_specs=P("tp", None, "ctx"),
        check_vma=False,
    )
```

```python
import functools
import math

import jax
import jax.numpy as jnp
from jax import lax
from jax.experimental import pallas as pl
from jax.experimental.pallas import tpu as pltpu
from jax.sharding import PartitionSpec as P


MAXB = 128
GROUP = 8
AHEAD = 32
COST = 10**10
NEG = -1e30
LOG2E = math.log2(math.e)
F32 = jnp.float32
BF16 = jnp.bfloat16

NT = (((1,), (1,)), ((), ()))


def request_kernel(owned, rows, block_len, round_ref, slot_ref, len_ref, q_ref, out_ref, count):
    me = lax.axis_index("ctx")
    for r in range(owned):
        count[r] = 0

    shift = MAXB.bit_length() - 1

    def tally(s, carry):
        local = lax.shift_right_arithmetic(slot_ref[s], shift) - me * owned
        local = jnp.where((local >= 0) & (local < owned), local, owned)
        count[local] = count[local] + 1
        return carry

    lax.fori_loop(0, slot_ref.shape[0], tally, 0, unroll=8)
    seen = jnp.int32(0)
    pick = jnp.int32(-1)
    for r in range(owned):
        blocks = lax.div(len_ref[me * owned + r] + (block_len - 1), block_len)
        lent = count[r] < blocks
        pick = jnp.where(lent & (seen == round_ref[0]), r, pick)
        seen = seen + lent.astype(jnp.int32)
    row = lax.broadcasted_iota(jnp.int32, (16, 128), 0)
    info = jnp.where(row == 0, seen, pick).astype(F32).astype(BF16)
    body = q_ref[jnp.maximum(pick, 0)]
    for c in range(out_ref.shape[0]):
        out_ref[c, pl.ds(0, rows), :] = body
        out_ref[c, pl.ds(rows, 16), :] = info


def attend(
    foreign, owned, kv, group, slot_ref, len_ref, query_of, first,
    k_hbm, v_hbm, kbuf, vbuf, ksem, vsem, order, sbuf, hbuf, m_acc, l_acc, a_acc,
):
    me = lax.axis_index("ctx")
    width, head = kbuf.shape[1:]
    block_len = width // kv
    rows = m_acc.shape[1]
    heads = group * kv
    coef = head ** -0.5 * LOG2E
    shift = MAXB.bit_length() - 1
    low, past = me * owned, (me + 1) * owned

    def begin(s, n):
        code = slot_ref[s]
        r = lax.shift_right_arithmetic(code, shift)
        inside = (r >= low) & (r < past)
        mine = (code >= 0) & (jnp.logical_not(inside) if foreign else inside)
        order[n] = s
        return n + mine.astype(jnp.int32)

    n = lax.fori_loop(0, slot_ref.shape[0], begin, jnp.int32(0), unroll=8)

    def fetch(i, carry):
        s = order[i]
        pltpu.make_async_copy(k_hbm.at[s], kbuf.at[i], ksem.at[i]).start()
        pltpu.make_async_copy(v_hbm.at[s], vbuf.at[i], vsem.at[i]).start()
        return carry

    lax.fori_loop(0, jnp.minimum(n, AHEAD), fetch, 0)
    first()
    col = lax.broadcasted_iota(jnp.int32, (2 * rows, width), 1)
    row = lax.broadcasted_iota(jnp.int32, (2 * rows, width), 0)
    same = (col % kv) == (row % heads) // group
    place = jnp.where(same, col, width * 2)
    none = jnp.zeros((rows, head), BF16)

    def at(i):
        slot = jnp.minimum(i, n - 1)
        code = slot_ref[order[slot]]
        r = lax.shift_right_arithmetic(code, shift)
        valid = jnp.clip(len_ref[r] - (code - r * MAXB) * block_len, 0, block_len)
        valid = jnp.where(i < n, valid, 0) * kv
        return slot, (jnp.int32(0) if foreign else r - low), valid

    def wait(base, source, buf, sem):
        for g in range(GROUP):
            i = base + g

            @pl.when(i < n)
            def _():
                pltpu.make_async_copy(source.at[0], buf.at[i], sem.at[i]).wait()

    def score(base, side):
        for p in range(GROUP // 2):
            sa, ea, va = at(base + 2 * p)
            sb, eb, vb = at(base + 2 * p + 1)
            left = jnp.concatenate(
                [
                    jnp.concatenate([query_of(ea), none], axis=1),
                    jnp.concatenate([none, query_of(eb)], axis=1),
                ],
                axis=0,
            )
            right = jnp.concatenate([kbuf[sa], kbuf[sb]], axis=1)
            raw = lax.dot_general(left, right, NT, preferred_element_type=F32)
            for half, valid in ((0, va), (1, vb)):
                part = slice(half * rows, (half + 1) * rows)
                masked = jnp.where(place[part] < valid, raw[part], NEG)
                sbuf[side, p, part, :] = masked
                high = jnp.max(masked, axis=1, keepdims=True)
                hbuf[side, p, part, :] = jnp.broadcast_to(high, (rows, 128))

    def mix(base, side):
        for p in range(GROUP // 2):
            sa, ea, _ = at(base + 2 * p)
            sb, eb, _ = at(base + 2 * p + 1)
            high = hbuf[side, p]
            total = None
            pieces = []
            for c in range(width // 128):
                w = jnp.exp2((sbuf[side, p, :, c * 128 : (c + 1) * 128] - high) * coef).astype(BF16)
                pieces.append(w)
                rounded = w.astype(F32)
                total = rounded if total is None else total + rounded
            weights = jnp.concatenate(pieces, axis=1)
            right = jnp.concatenate([vbuf[sa], vbuf[sb]], axis=1)
            summed = jnp.dot(weights, right, preferred_element_type=F32)
            for half, e in ((0, ea), (1, eb)):
                part = slice(half * rows, (half + 1) * rows)
                before = m_acc[e]
                peak = jnp.maximum(before, high[part])
                keep = jnp.exp2((before - peak) * coef)
                add = jnp.exp2((high[part] - peak) * coef)
                m_acc[e] = peak
                l_acc[e] = l_acc[e] * keep + total[part] * add
                a_acc[e] = a_acc[e] * keep + summed[part, half * head : (half + 1) * head] * add

    def step(it, carry):
        base = it * GROUP
        lax.fori_loop(jnp.minimum(base + AHEAD, n), jnp.minimum(base + GROUP + AHEAD, n), fetch, 0)
        wait(base + GROUP, k_hbm, kbuf, ksem)
        wait(base, v_hbm, vbuf, vsem)
        side = lax.rem(it, 2)
        score(base + GROUP, 1 - side)
        mix(base, side)
        return carry

    @pl.when(n > 0)
    def _():
        wait(0, k_hbm, kbuf, ksem)
        score(0, 0)
        lax.fori_loop(0, lax.div(n + GROUP - 1, GROUP), step, 0)


def own_kernel(
    owned, steps, kv, group, slot_ref, len_ref, q_ref, nk_hbm, nv_hbm, k_hbm, v_hbm,
    out_ref, lse_ref, nk_ref, nv_ref, nsem, kbuf, vbuf, ksem, vsem, order, sbuf, hbuf, m_acc, l_acc, a_acc,
):
    rows, head = q_ref.shape[1:]
    heads = kv * group
    coef = head ** -0.5 * LOG2E
    fresh = nk_ref.shape[0]
    nk_copy = pltpu.make_async_copy(nk_hbm, nk_ref, nsem.at[0])
    nv_copy = pltpu.make_async_copy(nv_hbm, nv_ref, nsem.at[1])
    nk_copy.start()
    nv_copy.start()
    col = lax.broadcasted_iota(jnp.int32, (rows, fresh), 1)
    row = lax.broadcasted_iota(jnp.int32, (rows, fresh), 0)
    seen = ((col % kv) == (row % heads) // group) & (lax.div(col, kv) % steps <= lax.div(row, heads))
    lane = lax.broadcasted_iota(jnp.int32, (rows, 128), 1)

    def first():
        nk_copy.wait()
        nv_copy.wait()
        nk = nk_ref[...]
        nv = nv_ref[...]
        for r in range(owned):
            scores = lax.dot_general(q_ref[r], nk, NT, preferred_element_type=F32)
            ok = seen & (lax.div(col, kv * steps) == r)
            scores = jnp.where(ok, scores, NEG)
            high = jnp.max(scores, axis=1, keepdims=True)
            weights = jnp.where(ok, jnp.exp2((scores - high) * coef), 0.0).astype(BF16)
            total = jnp.sum(weights.astype(F32), axis=1, keepdims=True)
            m_acc[r] = jnp.broadcast_to(high, (rows, 128))
            l_acc[r] = jnp.where(lane == 0, total, 0.0)
            a_acc[r] = jnp.dot(weights, nv, preferred_element_type=F32)

    attend(
        False, owned, kv, group, slot_ref, len_ref, lambda e: q_ref[e], first,
        k_hbm, v_hbm, kbuf, vbuf, ksem, vsem, order, sbuf, hbuf, m_acc, l_acc, a_acc,
    )
    table = jnp.zeros((rows, 128), F32)
    for r in range(owned):
        total = jnp.sum(l_acc[r], axis=1, keepdims=True)
        out_ref[r] = (a_acc[r] / total).astype(BF16)
        table = jnp.where(lane % 32 == r, m_acc[r] * coef + jnp.log(total) * LOG2E, table)
    lse_ref[...] = table


def lent_kernel(
    owned, kv, group, slot_ref, len_ref, got_ref, own_ref, lse_ref, k_hbm, v_hbm,
    out_ref, info_ref, kbuf, vbuf, ksem, vsem, order, sbuf, hbuf, m_acc, l_acc, a_acc,
):
    rows, head = out_ref.shape[1:]
    coef = head ** -0.5 * LOG2E
    me = lax.axis_index("ctx")

    shift = MAXB.bit_length() - 1

    def find(s, rid):
        code = slot_ref[s]
        r = lax.shift_right_arithmetic(code, shift)
        inside = (r >= me * owned) & (r < (me + 1) * owned)
        return jnp.where((code >= 0) & jnp.logical_not(inside), r, rid)

    rid = lax.fori_loop(0, slot_ref.shape[0], find, jnp.int32(-1), unroll=8)
    owner = lax.div(jnp.maximum(rid, 0), owned)
    most = got_ref[0, pl.ds(rows, 16), :].astype(F32)
    for c in range(1, got_ref.shape[0]):
        most = jnp.maximum(most, got_ref[c, pl.ds(rows, 16), :].astype(F32))
    info_ref[0] = jnp.max(most[:1]).astype(jnp.int32)
    sent = jnp.max(got_ref[owner, pl.ds(rows, 16), :].astype(F32)[1:2]).astype(jnp.int32)
    info_ref[1] = (sent == lax.rem(rid, owned)).astype(jnp.int32)

    def first():
        m_acc[0] = jnp.full((rows, 128), NEG, F32)
        l_acc[0] = jnp.zeros((rows, 128), F32)
        a_acc[0] = jnp.zeros((rows, head), F32)
        out_ref[pl.ds(0, owned)] = own_ref[...]

    attend(
        True, owned, kv, group, slot_ref, len_ref, lambda e: got_ref[owner, pl.ds(0, rows), :], first,
        k_hbm, v_hbm, kbuf, vbuf, ksem, vsem, order, sbuf, hbuf, m_acc, l_acc, a_acc,
    )
    total = jnp.sum(l_acc[0], axis=1, keepdims=True)
    some = total > 0.0
    total = jnp.where(some, total, 1.0)
    out_ref[owned] = (a_acc[0] / total).astype(BF16)
    lse = jnp.where(some, m_acc[0] * coef + jnp.log(total) * LOG2E, NEG)
    lane = lax.broadcasted_iota(jnp.int32, (rows, 128), 1)
    table = jnp.where(lane % 32 == owned, lse, lse_ref[...])
    table = jnp.where(lane % 32 == owned + 1, rid.astype(F32), table)
    second = table - table.astype(BF16).astype(F32)
    third = second - second.astype(BF16).astype(F32)
    out_ref[owned + 1] = jnp.where(lane < 32, table, jnp.where(lane < 64, second, third)).astype(BF16)


def project_kernel(
    owned, steps, heads, sources, parts, *refs
):
    pieces = refs[:sources]
    w_hbm, send_ref, keep_ref, full, lse, flat, wbuf, wsem = refs[sources:]
    me = lax.axis_index("ctx")
    mine = lax.axis_index("tp")
    rows = steps * heads
    head = full.shape[1]
    span = owned * rows
    per = sources // parts
    copy = pltpu.make_async_copy(w_hbm, wbuf, wsem)
    copy.start()

    def spot(c):
        return (lax.div(c, per) ^ mine) * per + lax.rem(c, per)

    lane = lax.broadcasted_iota(jnp.int32, (rows, 128), 1)
    for d in range(sources):
        start = pl.multiple_of(spot(me ^ d) * span, span)
        full[pl.ds(start, span), :] = pieces[d][pl.ds(0, owned)].astype(F32).reshape(span, head)
    rids = []
    theirs = []
    for d in range(sources):
        packed = pieces[d][owned + 1].astype(F32)
        table = packed + pltpu.roll(packed, 96, 1) + pltpu.roll(packed, 64, 1)
        lse[me ^ d] = table
        theirs.append(jnp.sum(jnp.where(lane == owned, table, 0.0), axis=1, keepdims=True))
        rids.append(jnp.max(jnp.where(lane[:8] == owned + 1, table[:8], -1.0)).astype(jnp.int32))
    for d in range(sources):

        @pl.when(rids[d] >= 0)
        def _(d=d):
            c = lax.div(rids[d], owned)
            r = lax.rem(rids[d], owned)
            start = pl.multiple_of((spot(c) * owned + r) * rows, rows)
            table = lse[c]
            left = jnp.sum(jnp.where(lane == r, table, 0.0), axis=1, keepdims=True)
            right = theirs[d]
            peak = jnp.maximum(left, right)
            w_left = jnp.exp2(left - peak)
            w_right = jnp.exp2(right - peak)
            total = w_left + w_right
            full[pl.ds(start, rows), :] = full[pl.ds(start, rows), :] * (w_left / total) + pieces[
                d
            ][owned].astype(F32) * (w_right / total)
            lse[c] = jnp.where(lane == r, peak + jnp.log(total) * LOG2E, table)
    count = sources * owned * steps
    for h in range(heads):
        flat[:, h * head : (h + 1) * head] = full[pl.ds(h, count, stride=heads), :].astype(BF16)
    copy.wait()
    result = jnp.dot(flat[...], wbuf[...], preferred_element_type=F32).astype(BF16)
    kept = count // parts
    for b in range(parts):
        target = keep_ref if b % 2 == 0 else send_ref
        target[b // 2] = result[b * kept : (b + 1) * kept]


def smem():
    return pl.BlockSpec(memory_space=pltpu.SMEM)


def vmem():
    return pl.BlockSpec(memory_space=pltpu.VMEM)


def hbm():
    return pl.BlockSpec(memory_space=pltpu.HBM)


def in_hbm(x):
    return pltpu.with_memory_space_constraint(x, pltpu.HBM)


def per_device(
    queries, new_keys, new_values, key_pool, value_pool, slot_block, lengths, out_weight
):
    owned, steps, heads, head = queries.shape
    kv = new_keys.shape[2]
    group = heads // kv
    slots, block_len = key_pool.shape[:2]
    sources = lax.axis_size("ctx")
    parts = lax.axis_size("tp")
    rows = steps * heads
    cols = out_weight.shape[1]
    q = queries.reshape(owned, rows, head)
    nk = in_hbm(new_keys.reshape(owned * steps * kv, head))
    nv = in_hbm(new_values.reshape(owned * steps * kv, head))
    keys = in_hbm(key_pool.reshape(slots, block_len * kv, head))
    values = in_hbm(value_pool.reshape(slots, block_len * kv, head))
    weight = in_hbm(out_weight)

    def ask(turn):
        message = pl.pallas_call(
            functools.partial(request_kernel, owned, rows, block_len),
            out_shape=jax.ShapeDtypeStruct((sources, rows + 16, head), BF16),
            in_specs=[smem(), smem(), smem(), vmem()],
            out_specs=vmem(),
            scratch_shapes=[pltpu.SMEM((owned + 1,), jnp.int32)],
            name="ask",
        )(turn, slot_block, lengths, q)
        return lax.all_to_all(message, "ctx", split_axis=0, concat_axis=0, tiled=True)

    cost = pl.CostEstimate(flops=COST, bytes_accessed=key_pool.size * 4, transcendentals=0)

    def buffers(sets):
        return [
            pltpu.VMEM((slots, block_len * kv, head), BF16),
            pltpu.VMEM((slots, block_len * kv, head), BF16),
            pltpu.SemaphoreType.DMA((slots,)),
            pltpu.SemaphoreType.DMA((slots,)),
            pltpu.SMEM((slots + 1,), jnp.int32),
            pltpu.VMEM((2, GROUP // 2, 2 * rows, block_len * kv), F32),
            pltpu.VMEM((2, GROUP // 2, 2 * rows, 128), F32),
            pltpu.VMEM((sets, rows, 128), F32),
            pltpu.VMEM((sets, rows, 128), F32),
            pltpu.VMEM((sets, rows, head), F32),
        ]

    got = ask(jnp.zeros((1,), jnp.int32))
    own, lse = pl.pallas_call(
        functools.partial(own_kernel, owned, steps, kv, group),
        out_shape=(
            jax.ShapeDtypeStruct((owned, rows, head), BF16),
            jax.ShapeDtypeStruct((rows, 128), F32),
        ),
        in_specs=[smem(), smem(), vmem(), hbm(), hbm(), hbm(), hbm()],
        out_specs=(vmem(), vmem()),
        scratch_shapes=[
            pltpu.VMEM(nk.shape, BF16),
            pltpu.VMEM(nv.shape, BF16),
            pltpu.SemaphoreType.DMA((2,)),
        ]
        + buffers(owned),
        cost_estimate=cost,
        name="own",
        compiler_params=pltpu.CompilerParams(vmem_limit_bytes=40 * 2**20),
    )(slot_block, lengths, q, nk, nv, keys, values)

    def answer(got):
        return pl.pallas_call(
            functools.partial(lent_kernel, owned, kv, group),
            out_shape=(
                jax.ShapeDtypeStruct((owned + 2, rows, head), BF16),
                jax.ShapeDtypeStruct((2,), jnp.int32),
            ),
            in_specs=[smem(), smem(), vmem(), vmem(), vmem(), hbm(), hbm()],
            out_specs=(vmem(), smem()),
            scratch_shapes=buffers(1),
            cost_estimate=cost,
            name="lent",
            compiler_params=pltpu.CompilerParams(vmem_limit_bytes=40 * 2**20),
        )(slot_block, lengths, got, own, lse, keys, values)

    partial, info = answer(got)

    def more(state):
        return state[0] < state[1]

    def next_round(state):
        turn, rounds, held = state
        fresh, info = answer(ask(turn.reshape(1)))
        return turn + 1, rounds, jnp.where(info[1] > 0, fresh, held)

    _, _, partial = lax.while_loop(more, next_round, (jnp.int32(1), info[0], partial))

    pieces = [partial]
    for d in range(1, sources):
        bit = d & -d
        pieces.append(lax.ppermute(pieces[d ^ bit], "ctx", [(i, i ^ bit) for i in range(sources)]))
    count = sources * owned * steps
    kept = count // parts
    send, keep = pl.pallas_call(
        functools.partial(project_kernel, owned, steps, heads, sources, parts),
        out_shape=(
            jax.ShapeDtypeStruct((parts // 2, kept, cols), BF16),
            jax.ShapeDtypeStruct((parts // 2, kept, cols), BF16),
        ),
        in_specs=[vmem()] * sources + [hbm()],
        out_specs=(vmem(), vmem()),
        scratch_shapes=[
            pltpu.VMEM((sources * owned * rows, head), F32),
            pltpu.VMEM((sources, rows, 128), F32),
            pltpu.VMEM((count, heads * head), BF16),
            pltpu.VMEM(out_weight.shape, BF16),
            pltpu.SemaphoreType.DMA,
        ],
        name="project",
        compiler_params=pltpu.CompilerParams(vmem_limit_bytes=48 * 2**20),
    )(*pieces, weight)

    bit = 1
    while True:
        other = lax.ppermute(send, "tp", [(i, i ^ bit) for i in range(parts)])
        held = keep.astype(F32) + other.astype(F32)
        bit *= 2
        if bit == parts:
            break
        held = held.reshape((held.shape[0] // 2, 2) + held.shape[1:])
        send, keep = held[:, 1].astype(BF16), held[:, 0]
    return held.astype(BF16).reshape(kept // steps, steps, cols)


def solution(mesh):
    return jax.shard_map(
        per_device,
        mesh=mesh,
        in_specs=(
            P("ctx", None, "tp", None),
            P("ctx", None, "tp", None),
            P("ctx", None, "tp", None),
            P("ctx", None, "tp", None),
            P("ctx", None, "tp", None),
            P("ctx"),
            P(),
            P("tp", "ctx"),
        ),
        out_specs=P("tp", None, "ctx"),
        check_vma=False,
    )
```
